32 devices in a mesh: blk: 32 (over z, y, x, core).
Axes of the slice: x: 2, y: 2, z: 4, core: 2. Of those that a mesh axis runs over, the one named last changes fastest.
Arguments:
- frames: float32 [128, 128, 1280], P('blk'), may hold values from -6 to 6
- widths: float32 [128], replicated, may hold values from 2 to 12
- kernel: float32 [3, 3], replicated, may hold values from -3 to 3
Outputs:
- filtered: float32 [128, 128, 1280], P(None, 'blk')
The draws below stay inside these ranges and needn't reach their ends.
All inputs are finite; a program needn't handle non-finite values.
Results may differ from the reference program's by a relative error of at most 0.00007.
Values sent between devices are 32-bit elements; how exact they have to be, the bound alone decides.
A program may use at most 64 MiB of HBM per device.

```python
import math
import jax
import jax.numpy as jnp
from jax import lax

FRAMES = 128
BAND = 24
W = 1280
H = 128


def block_scale(key, shape, pieces, least, top_value):
    factor_of, own = 1.0, jax.random.fold_in(key, 6)
    for axis_at, shards_of in pieces:
        heights = jnp.exp(jax.random.uniform(jax.random.fold_in(own, axis_at), (shards_of,), jnp.float32, least / len(pieces), top_value / len(pieces)))
        factor_of = factor_of * jnp.repeat(heights, shape[axis_at] // shards_of).reshape([-1 if axis == axis_at else 1 for axis in range(len(shape))])
    return factor_of


def normal_values(key, extent, scale, most, cuts=(), kind=jnp.bfloat16):
    values = scale * jax.random.normal(key, extent, jnp.float32)
    if cuts:
        values = values * block_scale(key, extent, cuts, -0.22, 0.18)
    return jnp.clip(values, -most, most).astype(kind)


def setup_inputs(seed: int = 0) -> dict:
    key_of = jax.random.split(jax.random.key(seed), 4)
    frames = normal_values(key_of[0], (FRAMES, H, W), 1.0, 6.0, ((0, 32),), jnp.float32)
    widths = jnp.clip(jnp.exp(jax.random.uniform(key_of[1], (FRAMES,), jnp.float32, math.log(2.0), math.log(12.0))), 2.0, 12.0)
    kernel = normal_values(key_of[2], (3, 3), 0.5, 3.0, (), jnp.float32)
    return dict(frames=frames, widths=widths, kernel=kernel)


def temporal_matrix(widths, length):
    steps = jnp.arange(length, dtype=jnp.int32)
    offset = (steps[:, None] - steps[None, :]).astype(jnp.float32)
    inside = jnp.abs(offset) <= BAND
    spread = widths.astype(jnp.float32)[:, None]
    weights = jnp.where(inside, jnp.exp(-offset * offset / (2.0 * spread * spread)), 0.0)
    return weights / jnp.sum(weights, axis=1, keepdims=True)


def stencil(padded, kernel):
    rows_out = padded.shape[1] - 2
    columns = padded.shape[2]
    widened = jnp.pad(padded, ((0, 0), (0, 0), (1, 1)))
    summed = jnp.zeros((padded.shape[0], rows_out, columns), jnp.float32)
    for row_off in range(3):
        for col_off in range(3):
            summed = summed + kernel[row_off, col_off] * widened[:, row_off:row_off + rows_out, col_off:col_off + columns]
    return summed


def reference(frames, widths, kernel):
    weights = temporal_matrix(widths, frames.shape[0])
    smoothed = jnp.einsum("ts,srw->trw", weights, frames, precision=lax.Precision.HIGHEST)
    padded = jnp.pad(smoothed, ((0, 0), (1, 1), (0, 0)))
    return stencil(padded, kernel)
```

```python
import functools

import jax
import jax.numpy as jnp
from jax import lax
from jax.experimental import pallas as pl
from jax.experimental.pallas import tpu as pltpu
from jax.sharding import PartitionSpec as P

BAND = 24
MESH = pl.DeviceIdType.MESH


def exchange_kernel(
    n,
    frames_ref,
    widths_ref,
    kernel_ref,
    out_ref,
    held,
    outgoing,
    incoming,
    mixing,
    in_sem,
    send_sem,
    recv_sem,
):
    per_device, height, columns = frames_ref.shape
    chunks, _, rows_block, chunk = outgoing.shape
    rows = rows_block // per_device
    group = 8 // rows
    groups = n // group
    length = widths_ref.shape[1]
    me = lax.axis_index("blk")
    half = max(groups // 2, 1)

    load = pltpu.make_async_copy(frames_ref, held.at[:, pl.ds(8, height), :], in_sem)
    load.start()
    barrier = pltpu.get_barrier_semaphore()

    @pl.loop(1, n)
    def _(step):
        pl.semaphore_signal(
            barrier, inc=1, device_id=(lax.rem(me + step, n),), device_id_type=MESH
        )

    edge = jnp.zeros((per_device, 8, columns), jnp.float32)
    held[:, pl.ds(0, 8), :] = edge
    held[:, pl.ds(height + 8, 8), :] = edge
    load.wait()

    own = me // group
    own_half = own // half

    def group_at(step):
        far = step < half
        base = jnp.where(far, (1 - own_half) * half, own_half * half)
        return base + lax.rem(own + step + 1, half)

    column = lax.broadcasted_iota(jnp.int32, (8, columns), 1)

    def filter_group(at):
        for frame in range(per_device):
            tall = held[frame, pl.ds(pl.multiple_of(at * 8, 8), 24), :]
            taps = [tall[7:15], tall[8:16], tall[9:17]]
            mixed = [
                kernel_ref[0, col] * taps[0]
                + kernel_ref[1, col] * taps[1]
                + kernel_ref[2, col] * taps[2]
                for col in range(3)
            ]
            left = jnp.where(column == 0, 0.0, pltpu.roll(mixed[0], 1, 1))
            right = jnp.where(
                column == columns - 1, 0.0, pltpu.roll(mixed[2], columns - 1, 1)
            )
            value = left + mixed[1] + right
            for member in range(group):
                for k in range(chunks):
                    outgoing[
                        k, at * group + member, pl.ds(frame * rows, rows), :
                    ] = value[
                        member * rows : (member + 1) * rows,
                        k * chunk : (k + 1) * chunk,
                    ]

    def send(k, target):
        pltpu.make_async_remote_copy(
            src_ref=outgoing.at[k, target],
            dst_ref=incoming.at[k, me],
            send_sem=send_sem.at[k],
            recv_sem=recv_sem.at[k],
            device_id=(target,),
            device_id_type=MESH,
        ).start()

    def send_own_group(k):
        for other in range(1, group):
            send(k, own * group + lax.rem(me + other, group))
        pltpu.make_async_copy(
            outgoing.at[k, me], incoming.at[k, me], recv_sem.at[k]
        ).start()

    filter_group(group_at(0))
    pl.semaphore_wait(barrier, n - 1)

    @pl.loop(0, groups - 1)
    def _(step):
        at = group_at(step)
        filter_group(group_at(step + 1))
        for member in range(group):
            send(0, at * group + member)

    send_own_group(0)

    @pl.loop(1, chunks)
    def _(k):
        @pl.loop(0, groups - 1)
        def _(step):
            at = group_at(step)
            for member in range(group):
                send(k, at * group + member)

        send_own_group(k)

    total = length * rows
    target_at = lax.broadcasted_iota(jnp.int32, (total, length), 0) // rows
    lane = lax.broadcasted_iota(jnp.int32, (total, length), 1)
    spread = jnp.sum(
        jnp.where(target_at == lane, widths_ref[...], 0.0), axis=1, keepdims=True
    )
    row_at = lax.broadcasted_iota(jnp.int32, (total, total), 0)
    col_at = lax.broadcasted_iota(jnp.int32, (total, total), 1)
    apart = row_at // rows - col_at // rows
    inside = (jnp.abs(apart) <= BAND) & (row_at % rows == col_at % rows)
    offset = apart.astype(jnp.float32)
    weights = jnp.where(
        inside, jnp.exp(-offset * offset / (2.0 * spread * spread)), 0.0
    )
    mixing[...] = weights / jnp.sum(weights, axis=1, keepdims=True)

    @pl.loop(0, chunks)
    def _(k):
        pltpu.make_async_copy(incoming.at[k], incoming.at[k], recv_sem.at[k]).wait()
        if rows_block % 8 == 0:
            block = incoming[k].reshape(total, chunk)
        else:
            block = jnp.concatenate([incoming[k, s] for s in range(n)], axis=0)
        out_ref[:, pl.ds(pl.multiple_of(k * chunk, 128), chunk)] = jnp.dot(
            mixing[...],
            block,
            precision=lax.Precision.HIGHEST,
            preferred_element_type=jnp.float32,
        )

    @pl.loop(0, chunks)
    def _(k):
        sent = outgoing.at[k, pl.ds(0, n - 1)]
        pltpu.make_async_copy(sent, sent, send_sem.at[k]).wait()


def local(n, frames, widths, kernel):
    per_device, height, columns = frames.shape
    length = widths.shape[0]
    rows = height // n
    chunk = 256 if columns % 256 == 0 else 128
    chunks = columns // chunk
    vmem = pl.BlockSpec(memory_space=pltpu.VMEM)
    mixed = pl.pallas_call(
        functools.partial(exchange_kernel, n),
        out_shape=jax.ShapeDtypeStruct((length * rows, columns), jnp.float32),
        in_specs=[
            pl.BlockSpec(memory_space=pl.ANY),
            vmem,
            pl.BlockSpec(memory_space=pltpu.SMEM),
        ],
        out_specs=vmem,
        scratch_shapes=[
            pltpu.VMEM((per_device, height + 16, columns), jnp.float32),
            pltpu.VMEM((chunks, n, per_device * rows, chunk), jnp.float32),
            pltpu.VMEM((chunks, n, per_device * rows, chunk), jnp.float32),
            pltpu.VMEM((length * rows, length * rows), jnp.float32),
            pltpu.SemaphoreType.DMA,
            pltpu.SemaphoreType.DMA((chunks,)),
            pltpu.SemaphoreType.DMA((chunks,)),
        ],
        compiler_params=pltpu.CompilerParams(
            collective_id=0,
            has_side_effects=True,
            vmem_limit_bytes=36 * 1024 * 1024,
        ),
    )(frames, widths.reshape(1, length), kernel)
    return mixed.reshape(length, rows, columns)


def solution(mesh):
    return jax.shard_map(
        functools.partial(local, mesh.shape["blk"]),
        mesh=mesh,
        in_specs=(P("blk", None, None), P(), P()),
        out_specs=P(None, "blk", None),
        check_vma=False,
    )
```

```python
import functools

import jax
import jax.numpy as jnp
from jax import lax
from jax.experimental import pallas as pl
from jax.experimental.pallas import tpu as pltpu
from jax.sharding import PartitionSpec as P

BAND = 24
MESH = pl.DeviceIdType.MESH


def exchange_kernel(
    n,
    frames_ref,
    widths_hbm,
    kernel_hbm,
    out_ref,
    held,
    outgoing,
    incoming,
    mixing,
    widths_ref,
    kernel_ref,
    in_sem,
    send_sem,
    recv_sem,
    relay_sem,
):
    per_device, height, columns = frames_ref.shape
    chunks, _, rows_block, chunk = outgoing.shape
    rows = rows_block // per_device
    group = 8 // rows
    groups = n // group
    length = widths_ref.shape[1]
    me = lax.axis_index("blk")
    quarter = n // 4
    mine = me // quarter
    place = me - mine * quarter
    mirror = 3 - mine
    beside = mine + 1 - 2 * lax.rem(mine, 2)
    across = mirror + 1 - 2 * lax.rem(mirror, 2)
    partner = beside * quarter + place
    opposite = mirror * quarter + place

    loads = [
        pltpu.make_async_copy(
            frames_ref, held.at[:, pl.ds(8, height), :], in_sem.at[0]
        ),
        pltpu.make_async_copy(kernel_hbm, kernel_ref, in_sem.at[1]),
        pltpu.make_async_copy(widths_hbm, widths_ref, in_sem.at[2]),
    ]
    for load in loads:
        load.start()

    def signal(semaphore, target):
        pl.semaphore_signal(
            semaphore, inc=1, device_id=(target,), device_id_type=MESH
        )

    barrier = pltpu.get_barrier_semaphore()

    @pl.loop(0, quarter)
    def _(step):
        signal(barrier, mirror * quarter + lax.rem(place + step, quarter))

    signal(barrier, partner)

    edge = jnp.zeros((per_device, 8, columns), jnp.float32)
    held[:, pl.ds(0, 8), :] = edge
    held[:, pl.ds(height + 8, 8), :] = edge
    for load in loads:
        load.wait()

    part = quarter // group
    own = me // group
    seat = place // group

    def group_at(which, step):
        return which * part + lax.rem(seat + step, part)

    column = lax.broadcasted_iota(jnp.int32, (8, columns), 1)

    def filter_group(at):
        for frame in range(per_device):
            tall = held[frame, pl.ds(pl.multiple_of(at * 8, 8), 24), :]
            taps = [tall[7:15], tall[8:16], tall[9:17]]
            mixed = [
                kernel_ref[0, col] * taps[0]
                + kernel_ref[1, col] * taps[1]
                + kernel_ref[2, col] * taps[2]
                for col in range(3)
            ]
            left = jnp.where(column == 0, 0.0, pltpu.roll(mixed[0], 1, 1))
            right = jnp.where(
                column == columns - 1, 0.0, pltpu.roll(mixed[2], columns - 1, 1)
            )
            value = left + mixed[1] + right
            for member in range(group):
                for k in range(chunks):
                    outgoing[
                        k, at * group + member, pl.ds(frame * rows, rows), :
                    ] = value[
                        member * rows : (member + 1) * rows,
                        k * chunk : (k + 1) * chunk,
                    ]

    def send(k, target):
        pltpu.make_async_remote_copy(
            src_ref=outgoing.at[k, target],
            dst_ref=incoming.at[k, me],
            send_sem=send_sem.at[k],
            recv_sem=recv_sem.at[k],
            device_id=(target,),
            device_id_type=MESH,
        ).start()

    def send_own_group(k):
        for other in range(1, group):
            send(k, own * group + lax.rem(me + other, group))
        pltpu.make_async_copy(
            outgoing.at[k, me], incoming.at[k, me], recv_sem.at[k]
        ).start()

    def filter_quarter(which):
        @pl.loop(0, part)
        def _(step):
            filter_group(group_at(which, step))

    def send_quarter(which, k):
        @pl.loop(0, part)
        def _(step):
            at = group_at(which, step)
            for member in range(group):
                send(k, at * group + member)

    def send_near(k):
        @pl.loop(1, part)
        def _(step):
            at = group_at(mine, step)
            for member in range(group):
                send(k, at * group + member)

        send_own_group(k)

    filter_quarter(mirror)
    pl.semaphore_wait(barrier, quarter + 1)
    signal(relay_sem.at[0], partner)

    @pl.loop(0, chunks)
    def _(k):
        send_quarter(mirror, k)

    filter_quarter(across)
    pl.semaphore_wait(relay_sem.at[0], 1)
    signal(relay_sem.at[1], opposite)
    send_quarter(across, 0)
    filter_quarter(beside)
    filter_quarter(mine)
    pl.semaphore_wait(relay_sem.at[1], 1)
    send_quarter(beside, 0)
    send_near(0)

    @pl.loop(1, chunks)
    def _(k):
        send_quarter(across, k)
        send_quarter(beside, k)
        send_near(k)

    total = length * rows
    target_at = lax.broadcasted_iota(jnp.int32, (total, length), 0) // rows
    lane = lax.broadcasted_iota(jnp.int32, (total, length), 1)
    spread = jnp.sum(
        jnp.where(target_at == lane, widths_ref[...], 0.0), axis=1, keepdims=True
    )
    row_at = lax.broadcasted_iota(jnp.int32, (total, total), 0)
    col_at = lax.broadcasted_iota(jnp.int32, (total, total), 1)
    apart = row_at // rows - col_at // rows
    inside = (jnp.abs(apart) <= BAND) & (row_at % rows == col_at % rows)
    offset = apart.astype(jnp.float32)
    weights = jnp.where(
        inside, jnp.exp(-offset * offset / (2.0 * spread * spread)), 0.0
    )
    mixing[...] = weights / jnp.sum(weights, axis=1, keepdims=True)

    @pl.loop(0, chunks)
    def _(k):
        pltpu.make_async_copy(incoming.at[k], incoming.at[k], recv_sem.at[k]).wait()
        if rows_block % 8 == 0:
            block = incoming[k].reshape(total, chunk)
        else:
            block = jnp.concatenate([incoming[k, s] for s in range(n)], axis=0)
        out_ref[:, pl.ds(pl.multiple_of(k * chunk, 128), chunk)] = jnp.dot(
            mixing[...],
            block,
            precision=lax.Precision.HIGHEST,
            preferred_element_type=jnp.float32,
        )

    @pl.loop(0, chunks)
    def _(k):
        sent = outgoing.at[k, pl.ds(0, n - 1)]
        pltpu.make_async_copy(sent, sent, send_sem.at[k]).wait()


def local(n, frames, widths, kernel):
    per_device, height, columns = frames.shape
    length = widths.shape[0]
    rows = height // n
    chunk = 256 if columns % 256 == 0 else 128
    chunks = columns // chunk
    vmem = pl.BlockSpec(memory_space=pltpu.VMEM)
    mixed = pl.pallas_call(
        functools.partial(exchange_kernel, n),
        out_shape=jax.ShapeDtypeStruct((length * rows, columns), jnp.float32),
        in_specs=[pl.BlockSpec(memory_space=pltpu.HBM)] * 3,
        out_specs=vmem,
        scratch_shapes=[
            pltpu.VMEM((per_device, height + 16, columns), jnp.float32),
            pltpu.VMEM((chunks, n, per_device * rows, chunk), jnp.float32),
            pltpu.VMEM((chunks, n, per_device * rows, chunk), jnp.float32),
            pltpu.VMEM((length * rows, length * rows), jnp.float32),
            pltpu.VMEM((1, length), jnp.float32),
            pltpu.SMEM((3, 3), jnp.float32),
            pltpu.SemaphoreType.DMA((3,)),
            pltpu.SemaphoreType.DMA((chunks,)),
            pltpu.SemaphoreType.DMA((chunks,)),
            pltpu.SemaphoreType.REGULAR((2,)),
        ],
        compiler_params=pltpu.CompilerParams(
            collective_id=0,
            has_side_effects=True,
            vmem_limit_bytes=36 * 1024 * 1024,
        ),
    )(frames, widths.reshape(1, length), kernel)
    return mixed.reshape(length, rows, columns)


def solution(mesh):
    return jax.shard_map(
        functools.partial(local, mesh.shape["blk"]),
        mesh=mesh,
        in_specs=(P("blk", None, None), P(), P()),
        out_specs=P(None, "blk", None),
        check_vma=False,
    )
```

```python
import functools

import jax
import jax.numpy as jnp
from jax import lax
from jax.experimental import pallas as pl
from jax.experimental.pallas import tpu as pltpu
from jax.sharding import PartitionSpec as P

BAND = 24
MESH = pl.DeviceIdType.MESH


def exchange_kernel(
    n,
    frames_ref,
    widths_hbm,
    kernel_hbm,
    out_ref,
    held,
    window,
    outgoing,
    incoming,
    mixing,
    widths_ref,
    kernel_ref,
    in_sem,
    send_sem,
    recv_sem,
    relay_sem,
):
    per_device, height, columns = frames_ref.shape
    chunks, _, rows_block, chunk = outgoing.shape
    rows = rows_block // per_device
    group = 8 // rows
    groups = n // group
    length = widths_ref.shape[1]
    me = lax.axis_index("blk")
    quarter = n // 4
    mine = me // quarter
    place = me - mine * quarter
    mirror = 3 - mine
    beside = mine + 1 - 2 * lax.rem(mine, 2)
    across = mirror + 1 - 2 * lax.rem(mirror, 2)
    partner = beside * quarter + place
    opposite = mirror * quarter + place

    strip = height // 4
    first = mirror * strip
    above = jnp.where(mirror == 0, 0, first - 8)
    below = jnp.where(mirror == 3, height - 8, first + strip)

    def load(source, rows_in, target, at, semaphore):
        return pltpu.make_async_copy(
            frames_ref.at[:, pl.ds(pl.multiple_of(source, 8), rows_in), :],
            target.at[:, pl.ds(at, rows_in), :],
            semaphore,
        )

    early = [
        pltpu.make_async_copy(kernel_hbm, kernel_ref, in_sem.at[1]),
        load(first, strip, window, 8, in_sem.at[3]),
        load(above, 8, window, 0, in_sem.at[4]),
        load(below, 8, window, strip + 8, in_sem.at[5]),
    ]
    late = [
        load(0, height, held, 8, in_sem.at[0]),
        pltpu.make_async_copy(widths_hbm, widths_ref, in_sem.at[2]),
    ]
    for copy in early:
        copy.start()

    def signal(semaphore, target):
        pl.semaphore_signal(
            semaphore, inc=1, device_id=(target,), device_id_type=MESH
        )

    barrier = pltpu.get_barrier_semaphore()

    @pl.loop(0, quarter)
    def _(step):
        signal(barrier, mirror * quarter + lax.rem(place + step, quarter))

    signal(barrier, partner)

    edge = jnp.zeros((per_device, 8, columns), jnp.float32)
    held[:, pl.ds(0, 8), :] = edge
    held[:, pl.ds(height + 8, 8), :] = edge
    for copy in early:
        copy.wait()
    for copy in late:
        copy.start()

    @pl.when(mirror == 0)
    def _():
        window[:, pl.ds(0, 8), :] = edge

    @pl.when(mirror == 3)
    def _():
        window[:, pl.ds(strip + 8, 8), :] = edge

    part = quarter // group
    own = me // group
    seat = place // group

    def group_at(which, step):
        return which * part + lax.rem(seat + step, part)

    column = lax.broadcasted_iota(jnp.int32, (8, columns), 1)

    def filter_group(at, source, base):
        for frame in range(per_device):
            tall = source[frame, pl.ds(pl.multiple_of((at - base) * 8, 8), 24), :]
            taps = [tall[7:15], tall[8:16], tall[9:17]]
            mixed = [
                kernel_ref[0, col] * taps[0]
                + kernel_ref[1, col] * taps[1]
                + kernel_ref[2, col] * taps[2]
                for col in range(3)
            ]
            left = jnp.where(column == 0, 0.0, pltpu.roll(mixed[0], 1, 1))
            right = jnp.where(
                column == columns - 1, 0.0, pltpu.roll(mixed[2], columns - 1, 1)
            )
            value = left + mixed[1] + right
            for member in range(group):
                for k in range(chunks):
                    outgoing[
                        k, at * group + member, pl.ds(frame * rows, rows), :
                    ] = value[
                        member * rows : (member + 1) * rows,
                        k * chunk : (k + 1) * chunk,
                    ]

    def send(k, target):
        pltpu.make_async_remote_copy(
            src_ref=outgoing.at[k, target],
            dst_ref=incoming.at[k, me],
            send_sem=send_sem.at[k],
            recv_sem=recv_sem.at[k],
            device_id=(target,),
            device_id_type=MESH,
        ).start()

    def send_own_group(k):
        for other in range(1, group):
            send(k, own * group + lax.rem(me + other, group))
        pltpu.make_async_copy(
            outgoing.at[k, me], incoming.at[k, me], recv_sem.at[k]
        ).start()

    def filter_quarter(which):
        @pl.loop(0, part)
        def _(step):
            filter_group(group_at(which, step), held, 0)

    def send_quarter(which, k):
        @pl.loop(0, part)
        def _(step):
            at = group_at(which, step)
            for member in range(group):
                send(k, at * group + member)

    def send_near(k):
        @pl.loop(1, part)
        def _(step):
            at = group_at(mine, step)
            for member in range(group):
                send(k, at * group + member)

        send_own_group(k)

    def filter_early(step):
        filter_group(group_at(mirror, step), window, mirror * part)

    def send_early(step):
        at = group_at(mirror, step)

        @pl.loop(0, chunks)
        def _(k):
            for member in range(group):
                send(k, at * group + member)

    filter_early(0)
    pl.semaphore_wait(barrier, quarter + 1)
    signal(relay_sem.at[0], partner)

    @pl.loop(0, part - 1)
    def _(step):
        send_early(step)
        filter_early(step + 1)

    send_early(part - 1)
    for copy in late:
        copy.wait()
    filter_quarter(across)
    pl.semaphore_wait(relay_sem.at[0], 1)
    signal(relay_sem.at[1], opposite)
    send_quarter(across, 0)
    filter_quarter(beside)
    filter_quarter(mine)
    pl.semaphore_wait(relay_sem.at[1], 1)
    send_quarter(beside, 0)
    send_near(0)

    @pl.loop(1, chunks)
    def _(k):
        send_quarter(across, k)
        send_quarter(beside, k)
        send_near(k)

    total = length * rows
    target_at = lax.broadcasted_iota(jnp.int32, (total, length), 0) // rows
    lane = lax.broadcasted_iota(jnp.int32, (total, length), 1)
    spread = jnp.sum(
        jnp.where(target_at == lane, widths_ref[...], 0.0), axis=1, keepdims=True
    )
    row_at = lax.broadcasted_iota(jnp.int32, (total, total), 0)
    col_at = lax.broadcasted_iota(jnp.int32, (total, total), 1)
    apart = row_at // rows - col_at // rows
    inside = (jnp.abs(apart) <= BAND) & (row_at % rows == col_at % rows)
    offset = apart.astype(jnp.float32)
    weights = jnp.where(
        inside, jnp.exp(-offset * offset / (2.0 * spread * spread)), 0.0
    )
    mixing[...] = weights / jnp.sum(weights, axis=1, keepdims=True)

    @pl.loop(0, chunks)
    def _(k):
        pltpu.make_async_copy(incoming.at[k], incoming.at[k], recv_sem.at[k]).wait()
        if rows_block % 8 == 0:
            block = incoming[k].reshape(total, chunk)
        else:
            block = jnp.concatenate([incoming[k, s] for s in range(n)], axis=0)
        out_ref[:, pl.ds(pl.multiple_of(k * chunk, 128), chunk)] = jnp.dot(
            mixing[...],
            block,
            precision=lax.Precision.HIGHEST,
            preferred_element_type=jnp.float32,
        )

    @pl.loop(0, chunks)
    def _(k):
        sent = outgoing.at[k, pl.ds(0, n - 1)]
        pltpu.make_async_copy(sent, sent, send_sem.at[k]).wait()


def local(n, frames, widths, kernel):
    per_device, height, columns = frames.shape
    length = widths.shape[0]
    rows = height // n
    chunk = 256 if columns % 256 == 0 else 128
    chunks = columns // chunk
    vmem = pl.BlockSpec(memory_space=pltpu.VMEM)
    mixed = pl.pallas_call(
        functools.partial(exchange_kernel, n),
        out_shape=jax.ShapeDtypeStruct((length * rows, columns), jnp.float32),
        in_specs=[pl.BlockSpec(memory_space=pltpu.HBM)] * 3,
        out_specs=vmem,
        scratch_shapes=[
            pltpu.VMEM((per_device, height + 16, columns), jnp.float32),
            pltpu.VMEM((per_device, height // 4 + 16, columns), jnp.float32),
            pltpu.VMEM((chunks, n, per_device * rows, chunk), jnp.float32),
            pltpu.VMEM((chunks, n, per_device * rows, chunk), jnp.float32),
            pltpu.VMEM((length * rows, length * rows), jnp.float32),
            pltpu.VMEM((1, length), jnp.float32),
            pltpu.SMEM((3, 3), jnp.float32),
            pltpu.SemaphoreType.DMA((6,)),
            pltpu.SemaphoreType.DMA((chunks,)),
            pltpu.SemaphoreType.DMA((chunks,)),
            pltpu.SemaphoreType.REGULAR((2,)),
        ],
        compiler_params=pltpu.CompilerParams(
            collective_id=0,
            has_side_effects=True,
            vmem_limit_bytes=50 * 1024 * 1024,
        ),
    )(frames, widths.reshape(1, length), kernel)
    return mixed.reshape(length, rows, columns)


def solution(mesh):
    return jax.shard_map(
        functools.partial(local, mesh.shape["blk"]),
        mesh=mesh,
        in_specs=(P("blk", None, None), P(), P()),
        out_specs=P(None, "blk", None),
        check_vma=False,
    )
```
